256 devices in a mesh: model: 32 (over z, y), data: 8 (over x, core).
Axes of the slice: x: 4, y: 4, z: 8, core: 2. Of those that a mesh axis runs over, the one named last changes fastest.
Arguments:
- act_in: bfloat16 [65536, 1024], P('data')
- grad_out: bfloat16 [65536, 1024], P('data')
- w_up: bfloat16 [2, 1024, 4096], P(None, None, 'model')
- w_down: bfloat16 [2, 4096, 1024], P(None, 'model')
- master_up: float32 [2, 1024, 4096], P(None, 'data', 'model')
- master_down: float32 [2, 4096, 1024], P(None, ('model', 'data'))
- mom_up: float32 [2, 1024, 4096], P(None, 'data', 'model')
- mom_down: float32 [2, 4096, 1024], P(None, ('model', 'data'))
- var_up: float32 [2, 1024, 4096], P(None, 'data', 'model')
- var_down: float32 [2, 4096, 1024], P(None, ('model', 'data'))
- learn_rate: float32 [1], replicated
- clip_norm: float32 [1], replicated
Outputs:
- output 1: bfloat16 [2, 1024, 4096], P(None, None, 'model')
- output 2: bfloat16 [2, 4096, 1024], P(None, 'model')
- output 3: float32 [2, 1024, 4096], P(None, 'data', 'model')
- output 4: float32 [2, 4096, 1024], P(None, ('model', 'data'))
- output 5: float32 [2, 1024, 4096], P(None, 'data', 'model')
- output 6: float32 [2, 4096, 1024], P(None, ('model', 'data'))
- output 7: float32 [2, 1024, 4096], P(None, 'data', 'model')
- output 8: float32 [2, 4096, 1024], P(None, ('model', 'data'))
- output 9: float32 [1], replicated
All inputs are finite; a program needn't handle non-finite values.
Results may differ from the reference program's by a relative error of at most 0.00193806.
Values are sent between devices in bfloat16 or wider.
A program may use at most 768 MiB of HBM per device.

```python
import jax
import jax.numpy as jnp
from jax import lax

D = 1024
FF = 4096
TOKENS_DEV = 8192
DATA = 8
STEP = 10
ROWS = DATA * TOKENS_DEV

BETA_ONE = 0.9
BETA_TWO = 0.95
ADAM_EPS = 1e-8
NORM_EPS = 1e-6


def matmul(left_op, right_op):
    return jnp.dot(left_op, right_op, preferred_element_type=jnp.float32)


def gelu_fwd(z_low):
    return jax.nn.gelu(z_low.astype(jnp.float32)).astype(jnp.bfloat16)


def gelu_back(z_low, grad_low):
    _, back_fn = jax.vjp(jax.nn.gelu, z_low.astype(jnp.float32))
    return back_fn(grad_low.astype(jnp.float32))[0].astype(jnp.bfloat16)


def block_grads(x_blk, dy_blk, w_up, w_down):
    z_one = matmul(x_blk, w_up[0]).astype(jnp.bfloat16)
    act_one = gelu_fwd(z_one)
    hid_two = matmul(act_one, w_down[0]).astype(jnp.bfloat16)
    z_two = matmul(hid_two, w_up[1]).astype(jnp.bfloat16)
    act_two = gelu_fwd(z_two)
    grad_w4 = matmul(act_two.T, dy_blk)
    dact_two = matmul(dy_blk, w_down[1].T).astype(jnp.bfloat16)
    dz_two = gelu_back(z_two, dact_two)
    grad_w3 = matmul(hid_two.T, dz_two)
    dhid_two = matmul(dz_two, w_up[1].T).astype(jnp.bfloat16)
    grad_w2 = matmul(act_one.T, dhid_two)
    dact_one = matmul(dhid_two, w_down[0].T).astype(jnp.bfloat16)
    dz_one = gelu_back(z_one, dact_one)
    grad_w1 = matmul(x_blk.T, dz_one)
    return jnp.stack([grad_w1, grad_w3]), jnp.stack([grad_w2, grad_w4])


def adam_update(master_arr, mom_arr, var_arr, grad_arr, clip_scale, lr_val):
    scaled = clip_scale * grad_arr
    new_mom = BETA_ONE * mom_arr + (1.0 - BETA_ONE) * scaled
    new_var = BETA_TWO * var_arr + (1.0 - BETA_TWO) * scaled * scaled
    mom_hat = new_mom / (1.0 - BETA_ONE ** STEP)
    var_hat = new_var / (1.0 - BETA_TWO ** STEP)
    new_master = master_arr - lr_val * mom_hat / (jnp.sqrt(var_hat) + ADAM_EPS)
    return new_master, new_mom, new_var


def setup_inputs(seed: int = 0) -> dict:
    key_list = jax.random.split(jax.random.key(seed), 10)
    w_scale = D ** -0.5
    master_up = jax.random.normal(key_list[0], (2, D, FF), jnp.float32) * w_scale
    master_down = jax.random.normal(key_list[1], (2, FF, D), jnp.float32) * w_scale
    w_up = master_up.astype(jnp.bfloat16)
    w_down = master_down.astype(jnp.bfloat16)
    act_in = jax.random.normal(key_list[2], (ROWS, D), jnp.float32).astype(jnp.bfloat16)
    grad_out = jax.random.normal(key_list[3], (ROWS, D), jnp.float32).astype(jnp.bfloat16)
    est_up, est_down = block_grads(act_in[:TOKENS_DEV], grad_out[:TOKENS_DEV], w_up, w_down)
    sq_up = jnp.sum(est_up * est_up, axis=(1, 2)) / DATA
    sq_down = jnp.sum(est_down * est_down, axis=(1, 2)) / DATA
    est_norm = jnp.sqrt(jnp.sum(sq_up) + jnp.sum(sq_down))
    clip_frac = jax.random.uniform(key_list[4], (1,), jnp.float32, 0.3, 0.6)
    clip_norm = clip_frac * est_norm
    rms_up = clip_frac * jnp.sqrt(sq_up / (D * FF))
    rms_down = clip_frac * jnp.sqrt(sq_down / (D * FF))
    mom_up = jax.random.normal(key_list[5], (2, D, FF), jnp.float32) * rms_up[:, None, None]
    mom_down = jax.random.normal(key_list[6], (2, FF, D), jnp.float32) * rms_down[:, None, None]
    var_up = jax.random.uniform(key_list[7], (2, D, FF), jnp.float32, 0.25, 2.0) * (rms_up * rms_up)[:, None, None]
    var_down = jax.random.uniform(key_list[8], (2, FF, D), jnp.float32, 0.25, 2.0) * (rms_down * rms_down)[:, None, None]
    learn_rate = jax.random.uniform(key_list[9], (1,), jnp.float32, 0.1, 0.25) * w_scale
    return {"act_in": act_in, "grad_out": grad_out, "w_up": w_up, "w_down": w_down, "master_up": master_up, "master_down": master_down, "mom_up": mom_up, "mom_down": mom_down, "var_up": var_up, "var_down": var_down, "learn_rate": learn_rate, "clip_norm": clip_norm}


def reference(act_in, grad_out, w_up, w_down, master_up, master_down, mom_up, mom_down, var_up, var_down, learn_rate, clip_norm):
    x_blocks = act_in.reshape(DATA, TOKENS_DEV, D)
    dy_blocks = grad_out.reshape(DATA, TOKENS_DEV, D)

    def body_fn(carry_sum, block_pair):
        part_up, part_down = block_grads(block_pair[0], block_pair[1], w_up, w_down)
        return (carry_sum[0] + part_up, carry_sum[1] + part_down), None

    zero_sums = (jnp.zeros((2, D, FF), jnp.float32), jnp.zeros((2, FF, D), jnp.float32))
    grad_sums, _ = lax.scan(body_fn, zero_sums, (x_blocks, dy_blocks))
    grad_up = grad_sums[0] / DATA
    grad_down = grad_sums[1] / DATA
    sq_total = jnp.sum(grad_up * grad_up) + jnp.sum(grad_down * grad_down)
    norm_val = jnp.sqrt(sq_total)
    clip_scale = jnp.minimum(1.0, clip_norm[0] / (norm_val + NORM_EPS))
    lr_val = learn_rate[0]
    new_master_up, new_mom_up, new_var_up = adam_update(master_up, mom_up, var_up, grad_up, clip_scale, lr_val)
    new_master_down, new_mom_down, new_var_down = adam_update(master_down, mom_down, var_down, grad_down, clip_scale, lr_val)
    return (new_master_up.astype(jnp.bfloat16), new_master_down.astype(jnp.bfloat16), new_master_up, new_master_down, new_mom_up, new_mom_down, new_var_up, new_var_down, norm_val.reshape(1))
```

```python
import jax
import jax.numpy as jnp
from jax import lax
from jax.sharding import Mesh, PartitionSpec as P

STEP = 10
BETA_ONE = 0.9
BETA_TWO = 0.95
ADAM_EPS = 1e-8
NORM_EPS = 1e-6
F32 = jnp.float32
BF16 = jnp.bfloat16


def gelu_fwd(z_low):
    return jax.nn.gelu(z_low.astype(F32)).astype(BF16)


def gelu_back(z_low, grad_low):
    _, back_fn = jax.vjp(jax.nn.gelu, z_low.astype(F32))
    return back_fn(grad_low.astype(F32))[0].astype(BF16)


def adam_update(master_arr, mom_arr, var_arr, grad_arr, clip_scale, lr_val):
    scaled = clip_scale * grad_arr
    new_mom = BETA_ONE * mom_arr + (1.0 - BETA_ONE) * scaled
    new_var = BETA_TWO * var_arr + (1.0 - BETA_TWO) * scaled * scaled
    mom_hat = new_mom / (1.0 - BETA_ONE ** STEP)
    var_hat = new_var / (1.0 - BETA_TWO ** STEP)
    new_master = master_arr - lr_val * mom_hat / (jnp.sqrt(var_hat) + ADAM_EPS)
    return new_master, new_mom, new_var


def dot_nt(left, right):
    return lax.dot_general(left, right, (((1,), (1,)), ((), ())), preferred_element_type=F32)


def dot_nn(left, right):
    return lax.dot_general(left, right, (((1,), (0,)), ((), ())), preferred_element_type=F32)


def dot_tn(left, right):
    return lax.dot_general(left, right, (((0,), (0,)), ((), ())), preferred_element_type=F32)


def sum_rows(part):
    mine = lax.psum_scatter(part, "y", scatter_dimension=0, tiled=True).astype(BF16)
    return lax.all_gather(mine, "y", axis=0, tiled=True)


def solution(mesh):
    big = Mesh(mesh.devices.reshape(8, 4, 4, 2), ("z", "y", "x", "c"))
    model = ("z", "y")
    data = ("x", "c")
    spec_rows = P(data, None)
    spec_wup = P(None, None, model)
    spec_wdown = P(None, model, None)
    spec_sup = P(None, data, model)
    spec_sdown = P(None, model + data, None)
    spec_scalar = P(None)

    def local_step(act_in, grad_out, w_up, w_down, master_up, master_down, mom_up, mom_down, var_up, var_down, learn_rate, clip_norm):
        rows = act_in.shape[0] // 8
        start = lax.axis_index("z") * rows
        x_loc = lax.dynamic_slice_in_dim(act_in, start, rows, 0)
        dy_loc = lax.dynamic_slice_in_dim(grad_out, start, rows, 0)
        up_t = jnp.swapaxes(w_up, 1, 2)
        w1t = lax.all_gather(up_t[0], "z", axis=0, tiled=True)
        w2 = lax.all_gather(w_down[0], "z", axis=0, tiled=True)
        w3t = lax.all_gather(up_t[1], "z", axis=0, tiled=True)
        w4 = lax.all_gather(w_down[1], "z", axis=0, tiled=True)
        z_one = dot_nt(x_loc, w1t).astype(BF16)
        act_one = gelu_fwd(z_one)
        hid = sum_rows(dot_nn(act_one, w2))
        z_two = dot_nt(hid, w3t).astype(BF16)
        act_two = gelu_fwd(z_two)
        g4 = dot_tn(act_two, dy_loc)
        dz_two = gelu_back(z_two, dot_nt(dy_loc, w4).astype(BF16))
        g3 = dot_tn(dz_two, hid)
        err = sum_rows(dot_nn(dz_two, w3t))
        g2 = dot_tn(act_one, err)
        dz_one = gelu_back(z_one, dot_nt(err, w2).astype(BF16))
        g1 = dot_tn(dz_one, x_loc)
        every = ("z", "x", "c")

        def red_down(grad):
            return lax.psum_scatter(grad, every, scatter_dimension=0, tiled=True)

        def red_up(grad):
            blocks = grad.reshape(8, 128, 8, 128).transpose(0, 2, 1, 3).reshape(64 * 128, 128)
            return lax.psum_scatter(blocks, every, scatter_dimension=0, tiled=True).T

        grad_down = jnp.stack([red_down(g2), red_down(g4)]) / 8
        grad_up = jnp.stack([red_up(g1), red_up(g3)]) / 8
        sq_local = jnp.sum(grad_up * grad_up) + jnp.sum(grad_down * grad_down)
        norm_val = jnp.sqrt(lax.psum(sq_local, ("z", "y", "x", "c")))
        clip_scale = jnp.minimum(1.0, clip_norm[0] / (norm_val + NORM_EPS))
        lr_val = learn_rate[0]
        new_master_up, new_mom_up, new_var_up = adam_update(master_up, mom_up, var_up, grad_up, clip_scale, lr_val)
        new_master_down, new_mom_down, new_var_down = adam_update(master_down, mom_down, var_down, grad_down, clip_scale, lr_val)
        new_w_up = lax.all_gather(new_master_up.astype(BF16), data, axis=1, tiled=True)
        new_w_down = lax.all_gather(new_master_down.astype(BF16), data, axis=1, tiled=True)
        return (new_w_up, new_w_down, new_master_up, new_master_down, new_mom_up, new_mom_down, new_var_up, new_var_down, norm_val.reshape(1))

    return jax.shard_map(local_step, mesh=big, in_specs=(spec_rows, spec_rows, spec_wup, spec_wdown, spec_sup, spec_sdown, spec_sup, spec_sdown, spec_sup, spec_sdown, spec_scalar, spec_scalar), out_specs=(spec_wup, spec_wdown, spec_sup, spec_sdown, spec_sup, spec_sdown, spec_sup, spec_sdown, spec_scalar), check_vma=False)
```

```python
import jax
import jax.numpy as jnp
from jax import lax
from jax.experimental import pallas as pl
from jax.experimental.pallas import tpu as pltpu
from jax.sharding import Mesh, PartitionSpec as P

STEP = 10
BETA_ONE = 0.9
BETA_TWO = 0.95
ADAM_EPS = 1e-8
NORM_EPS = 1e-6
F32 = jnp.float32
BF16 = jnp.bfloat16
MESH = pl.DeviceIdType.MESH
ROOT = 0.7978845608028654
CUBE = 0.044715
VMEM_LIMIT = 67043328
WIDE = 1024
LANE = 128
SPAN = 512
TILE = 256
HALF = 64
SUB = 16
EIGHT = 8
FOUR = 4
PAIR = 2
TRIO = 3
SEVEN = 7
HALFROW = 32
SIX = 6


def nn(left, right):
    return lax.dot_general(left, right, (((1,), (0,)), ((), ())), preferred_element_type=F32)


def nt(left, right):
    return lax.dot_general(left, right, (((1,), (1,)), ((), ())), preferred_element_type=F32)


def tn(left, right):
    return lax.dot_general(left, right, (((0,), (0,)), ((), ())), preferred_element_type=F32)


def gelu_val(z):
    t = jnp.tanh(ROOT * (z + CUBE * (z * z * z)))
    return z * (0.5 * (1.0 + t))


def gelu_both(z):
    sq = z * z
    t = jnp.tanh(ROOT * (z + CUBE * (sq * z)))
    half = 0.5 * (1.0 + t)
    slope = half + z * (0.5 * (1.0 - t * t)) * (ROOT * (1.0 + (3.0 * CUBE) * sq))
    return z * half, slope


def adam_update(master_arr, mom_arr, var_arr, grad_arr, clip_scale, lr_val):
    scaled = clip_scale * grad_arr
    new_mom = BETA_ONE * mom_arr + (1.0 - BETA_ONE) * scaled
    new_var = BETA_TWO * var_arr + (1.0 - BETA_TWO) * scaled * scaled
    mom_hat = new_mom / (1.0 - BETA_ONE ** STEP)
    var_hat = new_var / (1.0 - BETA_TWO ** STEP)
    new_master = master_arr - lr_val * mom_hat / (jnp.sqrt(var_hat) + ADAM_EPS)
    return new_master, new_mom, new_var


def kernel(
    act_ref, dy_ref, wup_ref, wdn_ref, up_ref_a, up_ref_b, up_ref_c, down_ref_a, down_ref_b, down_ref_c, lr_ref, clip_ref,
    grad_out_ref, norm_out_ref, weight_out_ref,
    X, DY, W, Z1, A1, Z3, A3, H, E2, Q3, PART, Y1, Y2, G, DD, X1, X2, ZS, ZR, NW, NSRC, NRCV, NRCW, SUP, SDN, GOUT, NOUT,
    local_sem, send_sem, recv_sem, credit,
):
    z = lax.axis_index("z")
    y = lax.axis_index("y")
    x = lax.axis_index("x")
    c = lax.axis_index("c")
    other = 1 - c
    used = {"send": 0, "recv": 0}

    def recv_id():
        used["recv"] += 1
        return used["recv"] - 1

    def send(src, dst, rid, where):
        sid = used["send"]
        used["send"] += 1
        copy = pltpu.make_async_remote_copy(src_ref=src, dst_ref=dst, send_sem=send_sem.at[sid], recv_sem=recv_sem.at[rid], device_id=where, device_id_type=MESH)
        copy.start()
        return copy

    def got(dst, rid):
        pltpu.make_async_remote_copy(src_ref=dst, dst_ref=dst, send_sem=send_sem.at[0], recv_sem=recv_sem.at[rid], device_id={"c": other}, device_id_type=MESH).wait_recv()

    places = [
        (wup_ref.at[0], Q3.at[0]),
        (act_ref.at[pl.ds(z * WIDE, WIDE), :], X),
        (wdn_ref.at[0], W.at[1, z]),
        (wup_ref.at[1], Q3.at[1]),
        (wdn_ref.at[1], W.at[TRIO, z]),
        (dy_ref.at[pl.ds(z * WIDE, WIDE), :], DY),
    ]
    for k, ref in enumerate((up_ref_a, up_ref_b, up_ref_c)):
        places.append((ref, SUP.at[k]))
    for k, ref in enumerate((down_ref_a, down_ref_b, down_ref_c)):
        places.append((ref, SDN.at[k]))
    loads = [pltpu.make_async_copy(src, dst, local_sem.at[i]) for i, (src, dst) in enumerate(places)]
    for copy in loads:
        copy.start()

    barrier = pltpu.get_barrier_semaphore()
    for d in range(1, EIGHT):
        pl.semaphore_signal(barrier, inc=1, device_id={"z": (z + d) % EIGHT}, device_id_type=MESH)
    flat_me = y * EIGHT + x * PAIR + c

    def flat_device(k):
        return {"y": k // EIGHT, "x": (k // PAIR) % FOUR, "c": k % PAIR}

    def flat_body(d, _):
        pl.semaphore_signal(barrier, inc=1, device_id=flat_device((flat_me + d) % HALFROW), device_id_type=MESH)
        return 0

    lax.fori_loop(1, HALFROW, flat_body, 0)

    zr, zl = (z + 1) % EIGHT, (z + SEVEN) % EIGHT

    class WRing:
        def __init__(self, m):
            self.m = m
            self.rids = [recv_id() for _ in range(FOUR)]
            self.lids = [recv_id() for _ in range(FOUR)]
            self.dids = [recv_id() for _ in range(SEVEN)]
            self.sent = []

        def piece(self, idx, lo=0, n=HALF):
            return W.at[self.m, idx, pl.ds(c * HALF + lo, n), :]

        def far(self, idx):
            return W.at[self.m, idx, pl.ds(other * HALF, HALF), :]

        def push(self, idx, lo, n, rid, where):
            p = self.piece(idx, lo, n)
            self.sent.append(send(p, p, rid, where))

        def start(self):
            self.push(z, 0, HALF, self.rids[0], {"z": zr})
            self.push(z, 0, HALF, self.lids[0], {"z": zl})

        def step(self, s):
            if s < TRIO:
                a, b = (z + SEVEN - s) % EIGHT, (z + 1 + s) % EIGHT
                got(self.piece(a), self.rids[s])
                if s < PAIR:
                    self.push(a, 0, HALF, self.rids[s + 1], {"z": zr})
                else:
                    self.push(a, 0, HALFROW, self.rids[TRIO], {"z": zr})
                self.push(a, 0, HALF, self.dids[PAIR * s], {"c": other})
                got(self.piece(b), self.lids[s])
                if s < PAIR:
                    self.push(b, 0, HALF, self.lids[s + 1], {"z": zl})
                else:
                    self.push(b, HALFROW, HALFROW, self.lids[TRIO], {"z": zl})
                self.push(b, 0, HALF, self.dids[PAIR * s + 1], {"c": other})
            else:
                a = (z + FOUR) % EIGHT
                got(self.piece(a, 0, HALFROW), self.rids[TRIO])
                got(self.piece(a, HALFROW, HALFROW), self.lids[TRIO])
                self.push(a, 0, HALF, self.dids[SIX], {"c": other})

        def near(self, s):
            if s < TRIO:
                a, b = (z + SEVEN - s) % EIGHT, (z + 1 + s) % EIGHT
                got(self.far(a), self.dids[PAIR * s])
                got(self.far(b), self.dids[PAIR * s + 1])
                return [a, b]
            a = (z + FOUR) % EIGHT
            got(self.far(a), self.dids[SIX])
            return [a]

    class Rs4:
        def __init__(self, axis, me, src, one, two):
            self.axis, self.src, self.one, self.two = axis, src, one, two
            self.me, self.r, self.l, self.o = me, (me + 1) % FOUR, (me + TRIO) % FOUR, (me + PAIR) % FOUR
            self.ids = [recv_id() for _ in range(SIX)]
            self.sent = []

        def start(self):
            right, left = {self.axis: self.r}, {self.axis: self.l}
            self.sent.append(send(self.src(self.o, 0), self.one(0), self.ids[0], right))
            self.sent.append(send(self.src(self.o, 1), self.one(1), self.ids[1], left))
            self.sent.append(send(self.src(self.r, 1), self.two(0, 1), self.ids[TRIO], right))
            self.sent.append(send(self.src(self.l, 0), self.two(1, 0), self.ids[FOUR], left))

        def mid(self):
            got(self.one(0), self.ids[0])
            mine = self.src(self.r, 0)
            mine[...] = mine[...] + self.one(0)[...]
            self.sent.append(send(mine, self.two(0, 0), self.ids[PAIR], {self.axis: self.r}))
            got(self.one(1), self.ids[1])
            mine = self.src(self.l, 1)
            mine[...] = mine[...] + self.one(1)[...]
            self.sent.append(send(mine, self.two(1, 1), self.ids[5], {self.axis: self.l}))

        def fin(self, h):
            got(self.two(0, h), self.ids[PAIR + h])
            got(self.two(1, h), self.ids[FOUR + h])
            return self.src(self.me, h)[...] + self.two(0, h)[...] + self.two(1, h)[...]

    class Ag4:
        def __init__(self, axis, me, buf):
            self.axis, self.buf = axis, buf
            self.me, self.r, self.l, self.o = me, (me + 1) % FOUR, (me + TRIO) % FOUR, (me + PAIR) % FOUR
            self.ids = [recv_id() for _ in range(SIX)]
            self.sent = []

        def push(self, j, h, rid, to):
            p = self.buf(j, h)
            self.sent.append(send(p, p, rid, {self.axis: to}))

        def start(self):
            self.push(self.me, 0, self.ids[0], self.r)
            self.push(self.me, 1, self.ids[TRIO], self.l)
            self.push(self.me, 1, self.ids[1], self.r)
            self.push(self.me, 0, self.ids[PAIR], self.l)

        def fwd(self):
            got(self.buf(self.l, 0), self.ids[0])
            self.push(self.l, 0, self.ids[FOUR], self.r)
            got(self.buf(self.r, 1), self.ids[TRIO])
            self.push(self.r, 1, self.ids[5], self.l)

        def fin(self):
            got(self.buf(self.l, 1), self.ids[1])
            got(self.buf(self.r, 0), self.ids[PAIR])
            got(self.buf(self.o, 0), self.ids[FOUR])
            got(self.buf(self.o, 1), self.ids[5])

    def done(*things):
        for thing in things:
            for copy in thing.sent:
                copy.wait_send()
            thing.sent = []

    def rows_of(ref, p):
        return ref[p].reshape(SPAN, WIDE)

    def first_slice(j):
        def body(i, _):
            rows = pl.ds(pl.multiple_of(i * TILE, TILE), TILE)
            low = nt(X[rows, :], W[0, j]).astype(BF16)
            Z1[j, rows, :] = low
            A1[j, rows, :] = gelu_val(low.astype(F32)).astype(BF16)
            return 0

        lax.fori_loop(0, FOUR, body, 0)

    def partial(p, lhs, m):
        def body(n, _):
            cols = pl.ds(pl.multiple_of(n * TILE, TILE), TILE)
            rhs = W[m, :, :, cols].reshape(WIDE, TILE)
            left = jnp.concatenate([lhs[k, p * SPAN:(p + 1) * SPAN, :] for k in range(EIGHT)], axis=1)
            PART[p, :, :, cols] = nn(left, rhs).reshape(FOUR, LANE, TILE)
            return 0

        lax.fori_loop(0, FOUR, body, 0)

    def err_three(p):
        def body(n, _):
            val = nt(DY[p * SPAN:(p + 1) * SPAN, :], W[TRIO, pl.ds(PAIR * n, PAIR)].reshape(TILE, WIDE)).astype(BF16)
            Q3[PAIR * n, p * SPAN:(p + 1) * SPAN, :] = val[:, :LANE]
            Q3[PAIR * n + 1, p * SPAN:(p + 1) * SPAN, :] = val[:, LANE:]
            return 0

        lax.fori_loop(0, FOUR, body, 0)

    def block_two(p):
        def body(n, _):
            low = nt(rows_of(H, p), W[PAIR, pl.ds(PAIR * n, PAIR)].reshape(TILE, WIDE)).astype(BF16)
            for k in range(PAIR):
                part = low[:, k * LANE:(k + 1) * LANE].astype(F32)
                val, slope = gelu_both(part)
                A3[PAIR * n + k, p * SPAN:(p + 1) * SPAN, :] = val.astype(BF16)
                err = Q3[PAIR * n + k, p * SPAN:(p + 1) * SPAN, :].astype(F32)
                Q3[PAIR * n + k, p * SPAN:(p + 1) * SPAN, :] = (err * slope).astype(BF16)
            return 0

        lax.fori_loop(0, FOUR, body, 0)

    def back_one(p):
        def body(n, _):
            low = nt(rows_of(E2, p), W[1, pl.ds(PAIR * n, PAIR)].reshape(TILE, WIDE)).astype(BF16)
            for k in range(PAIR):
                zed = Z1[PAIR * n + k, p * SPAN:(p + 1) * SPAN, :].astype(F32)
                _, slope = gelu_both(zed)
                err = low[:, k * LANE:(k + 1) * LANE].astype(F32)
                Z3[PAIR * n + k, p * SPAN:(p + 1) * SPAN, :] = (err * slope).astype(BF16)
            return 0

        lax.fori_loop(0, FOUR, body, 0)

    def weight_grad(slot, hid, lo, size, other_side, down, first, last, add):
        def body(step, _):
            n = step // PAIR
            half = step % PAIR
            cols = pl.ds(pl.multiple_of(n * TILE, TILE), TILE)
            right = other_side(cols)
            for q in range(PAIR):
                base = half * FOUR + q * PAIR
                left = jnp.concatenate([hid[base, lo:lo + size, :], hid[base + 1, lo:lo + size, :]], axis=1)
                val = tn(left, right)
                for k in range(PAIR):
                    blk = val[k * LANE:(k + 1) * LANE, :]
                    for e in range(PAIR):
                        sub = blk[:, e * LANE:(e + 1) * LANE]
                        if down:
                            lane = pl.ds(pl.multiple_of((PAIR * n + e) * SUB, SUB), SUB)
                            for b in range(EIGHT):
                                old = G[slot, base + k, b // PAIR, b % PAIR, lane, :] if add else 0.0
                                G[slot, base + k, b // PAIR, b % PAIR, lane, :] = old + sub[b * SUB:(b + 1) * SUB, :]
                        else:
                            old = G[slot, base + k, n, e] if add else 0.0
                            G[slot, base + k, n, e] = old + sub
            return 0

        lax.fori_loop(PAIR * first, PAIR * last, body, 0)

    class GradPart:
        def __init__(self, k, u):
            self.k, self.u, self.slot = k, u, k % PAIR
            self.did = recv_id()
            self.zid = recv_id()
            slot = self.slot
            rows = pl.ds(HALF * u, HALF)
            self.rows = rows
            self.rs = Rs4("x", x, lambda j, h: G.at[slot, pl.ds(FOUR * h, FOUR), j, c, rows], lambda d: X1.at[k, u, d], lambda d, h: X2.at[k, u, d, h])
            self.sent = []
            self.zsent = []

        def d2d(self):
            if self.k >= PAIR:
                pl.semaphore_wait(credit.at[self.slot, self.u], 1)
            self.sent.append(send(G.at[self.slot, :, :, other, self.rows], DD.at[self.slot, self.u], self.did, {"c": other}))

        def xs(self):
            got(DD.at[self.slot, self.u], self.did)
            slot, u, rows = self.slot, self.u, self.rows

            def body(i, _):
                mine = G.at[slot, i, :, c, rows]
                mine[...] = mine[...] + DD[slot, u, i]
                return 0

            lax.fori_loop(0, EIGHT, body, 0)
            if self.k < PAIR:
                pl.semaphore_signal(credit.at[slot, u], inc=1, device_id={"c": other}, device_id_type=MESH)
            self.rs.start()

        def xm(self):
            self.rs.mid()

        def xf(self):
            for h in range(PAIR):
                ZS[self.slot, self.u, FOUR * h:FOUR * h + FOUR] = self.rs.fin(h)
            for d in (FOUR, TRIO, 5, PAIR, SIX, 1, SEVEN):
                to = (z + d) % EIGHT
                self.zsent.append(send(ZS.at[self.slot, self.u, to], ZR.at[self.k, self.u, d - 1], self.zid, {"z": to}))

        def zf(self):
            got(ZR.at[self.k, self.u], self.zid)
            total = ZS[self.slot, self.u, z]
            for d in range(SEVEN):
                total = total + ZR[self.k, self.u, d]
            total = total * 0.125
            GOUT[self.k, self.rows, :] = total
            sq = total * total
            return jnp.sum(sq.reshape(EIGHT, EIGHT, LANE), axis=0)

        def free_g(self):
            done(self, self.rs)

        def free_z(self):
            for copy in self.zsent:
                copy.wait_send()
            self.zsent = []

    w1, w2, w3, w4 = (WRing(m) for m in range(FOUR))
    rs_h = [Rs4("y", y, lambda j, h, p=p: PART.at[p, j, pl.ds(HALF * h, HALF), :], lambda d, p=p: Y1.at[0, p, d], lambda d, h, p=p: Y2.at[0, p, d, h]) for p in range(PAIR)]
    rs_e = [Rs4("y", y, lambda j, h, p=p: PART.at[p, j, pl.ds(HALF * h, HALF), :], lambda d, p=p: Y1.at[1, p, d], lambda d, h, p=p: Y2.at[1, p, d, h]) for p in range(PAIR)]
    ag_h = [Ag4("y", y, lambda j, h, p=p: H.at[p, j, pl.ds(HALF * h, HALF), :]) for p in range(PAIR)]
    ag_e = [Ag4("y", y, lambda j, h, p=p: E2.at[p, j, pl.ds(HALF * h, HALF), :]) for p in range(PAIR)]
    gs = [[GradPart(k, u) for u in range(PAIR)] for k in range(FOUR)]

    loads[0].wait()
    W[0, z] = Q3[0].T
    loads[1].wait()
    first_slice(z)
    loads[PAIR].wait()
    pl.semaphore_wait(barrier, 38)
    w1.start()
    w2.start()
    loads[TRIO].wait()
    W[PAIR, z] = Q3[1].T
    loads[FOUR].wait()
    for s in range(FOUR):
        w1.step(s)
        w2.step(s)
        if s == PAIR:
            w3.start()
            w4.start()
        for j in w1.near(s):
            first_slice(j)
    for s in range(FOUR):
        w2.near(s)
    partial(0, A1, 1)
    rs_h[0].start()
    w3.step(0)
    w4.step(0)
    partial(1, A1, 1)
    rs_h[1].start()
    w3.step(1)
    w4.step(1)
    rs_h[0].mid()
    w3.step(PAIR)
    w4.step(PAIR)
    loads[5].wait()
    rs_h[1].mid()
    w3.step(TRIO)
    w4.step(TRIO)
    for s in range(FOUR):
        w4.near(s)
    err_three(0)
    for h in range(PAIR):
        H[0, y, HALF * h:HALF * h + HALF, :] = rs_h[0].fin(h).astype(BF16)
    ag_h[0].start()
    err_three(1)
    for s in range(FOUR):
        w3.near(s)
    for h in range(PAIR):
        H[1, y, HALF * h:HALF * h + HALF, :] = rs_h[1].fin(h).astype(BF16)
    ag_h[0].fwd()
    ag_h[1].start()
    ag_h[0].fin()
    block_two(0)
    ag_h[1].fwd()
    done(rs_h[0])
    partial(0, Q3, PAIR)
    rs_e[0].start()
    ag_h[1].fin()
    block_two(1)
    done(rs_h[1])
    partial(1, Q3, PAIR)
    rs_e[1].start()
    rs_e[0].mid()
    weight_grad(0, A3, 0, WIDE, lambda cols: DY[:, cols], True, 0, PAIR, False)
    gs[0][0].d2d()
    weight_grad(0, A3, 0, WIDE, lambda cols: DY[:, cols], True, PAIR, FOUR, False)
    gs[0][1].d2d()
    gs[0][0].xs()
    weight_grad(1, Q3, 0, WIDE, lambda cols: H[:, :, :, cols].reshape(WIDE, TILE), False, 0, FOUR, False)
    gs[0][1].xs()
    gs[1][0].d2d()
    gs[1][1].d2d()
    rs_e[1].mid()
    gs[0][0].xm()
    gs[0][1].xm()
    gs[1][0].xs()
    gs[1][1].xs()
    for h in range(PAIR):
        E2[0, y, HALF * h:HALF * h + HALF, :] = rs_e[0].fin(h).astype(BF16)
    ag_e[0].start()
    gs[0][0].xf()
    gs[0][1].xf()
    for h in range(PAIR):
        E2[1, y, HALF * h:HALF * h + HALF, :] = rs_e[1].fin(h).astype(BF16)
    ag_e[0].fwd()
    ag_e[1].start()
    gs[1][0].xm()
    gs[1][1].xm()
    gs[0][0].free_g()
    gs[0][1].free_g()
    ag_e[0].fin()
    back_one(0)
    ag_e[1].fwd()
    weight_grad(0, A1, 0, SPAN, lambda cols: E2[0, :, :, cols].reshape(SPAN, TILE), True, 0, FOUR, False)
    gs[1][0].xf()
    gs[1][1].xf()
    gs[1][0].free_g()
    gs[1][1].free_g()
    weight_grad(1, Z3, 0, SPAN, lambda cols: X[:SPAN, cols], False, 0, FOUR, False)
    ag_e[1].fin()
    weight_grad(0, A1, SPAN, SPAN, lambda cols: E2[1, :, :, cols].reshape(SPAN, TILE), True, 0, PAIR, True)
    gs[PAIR][0].d2d()
    weight_grad(0, A1, SPAN, SPAN, lambda cols: E2[1, :, :, cols].reshape(SPAN, TILE), True, PAIR, FOUR, True)
    gs[PAIR][1].d2d()
    gs[PAIR][0].xs()
    back_one(1)
    gs[PAIR][1].xs()
    weight_grad(1, Z3, SPAN, SPAN, lambda cols: X[SPAN:, cols], False, 0, FOUR, True)
    gs[TRIO][0].d2d()
    gs[TRIO][1].d2d()
    gs[PAIR][0].xm()
    gs[TRIO][0].xs()
    gs[TRIO][1].xs()
    gs[PAIR][1].xm()
    sq = gs[0][0].zf() + gs[0][1].zf()
    gs[0][0].free_z()
    gs[0][1].free_z()
    gs[PAIR][0].xf()
    gs[TRIO][0].xm()
    gs[PAIR][1].xf()
    gs[TRIO][1].xm()
    sq = sq + gs[1][0].zf() + gs[1][1].zf()
    gs[1][0].free_z()
    gs[1][1].free_z()
    gs[TRIO][0].xf()
    sq = sq + gs[PAIR][0].zf()
    gs[TRIO][1].xf()
    sq = sq + gs[PAIR][1].zf() + gs[TRIO][0].zf()
    sq = sq + gs[TRIO][1].zf()

    grad_copy = pltpu.make_async_copy(GOUT, grad_out_ref, local_sem.at[0])
    grad_copy.start()
    nid, mid = recv_id(), recv_id()
    norm_sent = []
    NSRC[0] = sq
    for d in (FOUR, TRIO, 5, PAIR, SIX, 1, SEVEN):
        norm_sent.append(send(NSRC.at[0], NRCV.at[z], nid, {"z": (z + d) % EIGHT}))
    got(NRCV.at[pl.ds(0, SEVEN)], nid)
    NRCV[z] = sq
    part = NRCV[0]
    for k in range(1, EIGHT):
        part = part + NRCV[k]
    row = jnp.sum(part, axis=0, keepdims=True)
    row = jnp.broadcast_to(row, (EIGHT, LANE))
    NSRC[1] = row
    for d in range(1, HALFROW):
        norm_sent.append(send(NSRC.at[1], NRCW.at[flat_me], mid, flat_device((flat_me + d) % HALFROW)))
    got(NRCW.at[pl.ds(0, 31)], mid)
    NRCW[flat_me] = row
    total = jnp.sum(jnp.sum(NRCW[...], axis=0)[:1, :], axis=1, keepdims=True)
    norm_val = jnp.sqrt(total)
    NOUT[...] = jnp.broadcast_to(norm_val, (EIGHT, LANE))
    norm_copy = pltpu.make_async_copy(NOUT, norm_out_ref, local_sem.at[1])
    norm_copy.start()
    clip_scale = jnp.minimum(1.0, clip_ref[0] / (norm_val + NORM_EPS))
    lr_val = lr_ref[0]
    for copy in loads[SIX:]:
        copy.wait()
    for k in range(PAIR):
        new_master, _, _ = adam_update(SUP[0, k], SUP[1, k], SUP[PAIR, k], GOUT[TRIO - PAIR * k].T, clip_scale, lr_val)
        NW[x, c, k] = new_master.astype(BF16)
        flat = flatten(GOUT[PAIR - PAIR * k])
        new_master, _, _ = adam_update(SDN[0, k], SDN[1, k], SDN[PAIR, k], flat, clip_scale, lr_val)
        low = new_master.astype(BF16)
        for e in range(EIGHT):
            NW[x, c, PAIR + k, e * SUB:(e + 1) * SUB, :] = low[:, e * LANE:(e + 1) * LANE]
    ag_w = Ag4("x", x, lambda j, h: NW.at[j, c, pl.ds(PAIR * h, PAIR)])
    ag_w.start()
    pair = [recv_id() for _ in range(FOUR)]
    last = []

    def across(i, j):
        last.append(send(NW.at[j, c], NW.at[j, c], pair[i], {"c": other}))

    across(0, x)
    ag_w.fwd()
    ag_w.fin()
    for i, j in ((1, ag_w.l), (PAIR, ag_w.r), (TRIO, ag_w.o)):
        across(i, j)
    for i, j in ((0, x), (1, ag_w.l), (PAIR, ag_w.r), (TRIO, ag_w.o)):
        got(NW.at[j, other], pair[i])
    weight_copy = pltpu.make_async_copy(NW, weight_out_ref, local_sem.at[PAIR])
    weight_copy.start()

    for copy in last + norm_sent:
        copy.wait_send()
    done(w1, w2, w3, w4, ag_w, *rs_e, *ag_h, *ag_e)
    for parts in gs[PAIR:]:
        for part in parts:
            part.free_g()
            part.free_z()
    for copy in (grad_copy, norm_copy, weight_copy):
        copy.wait()


def flatten(grad):
    return jnp.concatenate([grad[e * SUB:(e + 1) * SUB, :] for e in range(EIGHT)], axis=1)


def finish_kernel(grad, norm, low, mau, mad, mou, mod, vau, vad, lr_ref, clip_ref, nwu, nwd, omau, omad, omou, omod, ovau, ovad, onorm):
    norm_val = norm[:1, :1]
    onorm[...] = norm_val
    clip_scale = jnp.minimum(1.0, clip_ref[0] / (norm_val + NORM_EPS))
    lr_val = lr_ref[0]
    for k in range(PAIR):
        omau[k], omou[k], ovau[k] = adam_update(mau[k], mou[k], vau[k], grad[TRIO - PAIR * k].T, clip_scale, lr_val)
        omad[k], omod[k], ovad[k] = adam_update(mad[k], mod[k], vad[k], flatten(grad[PAIR - PAIR * k]), clip_scale, lr_val)
        for b in range(EIGHT):
            nwu[k, b * LANE:(b + 1) * LANE, :] = low[b // PAIR, b % PAIR, k]
            nwd[k, b * SUB:(b + 1) * SUB, :] = flatten(low[b // PAIR, b % PAIR, PAIR + k])


SENDS = 330
RECVS = 250


def fused_step(act_in, grad_out, w_up, w_down, states, scalars):
    anywhere = pl.BlockSpec(memory_space=pl.ANY)
    near = pl.BlockSpec(memory_space=pltpu.VMEM)
    scalar = pl.BlockSpec(memory_space=pltpu.SMEM)
    act = pltpu.VMEM((EIGHT, WIDE, LANE), BF16)
    rows = pltpu.VMEM((PAIR, FOUR, LANE, WIDE), BF16)
    scratch = [
        pltpu.VMEM((WIDE, WIDE), BF16),
        pltpu.VMEM((WIDE, WIDE), BF16),
        pltpu.VMEM((FOUR, EIGHT, LANE, WIDE), BF16),
        act, act, act, act,
        rows, rows,
        act,
        pltpu.VMEM((PAIR, FOUR, LANE, WIDE), F32),
        pltpu.VMEM((PAIR, PAIR, PAIR, HALF, WIDE), F32),
        pltpu.VMEM((PAIR, PAIR, PAIR, PAIR, HALF, WIDE), F32),
        pltpu.VMEM((PAIR, EIGHT, FOUR, PAIR, LANE, LANE), F32),
        pltpu.VMEM((PAIR, PAIR, EIGHT, FOUR, HALF, LANE), F32),
        pltpu.VMEM((FOUR, PAIR, PAIR, FOUR, HALF, LANE), F32),
        pltpu.VMEM((FOUR, PAIR, PAIR, PAIR, FOUR, HALF, LANE), F32),
        pltpu.VMEM((PAIR, PAIR, EIGHT, HALF, LANE), F32),
        pltpu.VMEM((FOUR, PAIR, SEVEN, HALF, LANE), F32),
        pltpu.VMEM((FOUR, PAIR, FOUR, LANE, LANE), BF16),
        pltpu.VMEM((PAIR, EIGHT, LANE), F32),
        pltpu.VMEM((EIGHT, EIGHT, LANE), F32),
        pltpu.VMEM((HALFROW, EIGHT, LANE), F32),
        pltpu.VMEM((TRIO, PAIR, LANE, LANE), F32),
        pltpu.VMEM((TRIO, PAIR, SUB, WIDE), F32),
        pltpu.VMEM((FOUR, LANE, LANE), F32),
        pltpu.VMEM((EIGHT, LANE), F32),
        pltpu.SemaphoreType.DMA((12,)),
        pltpu.SemaphoreType.DMA((SENDS,)),
        pltpu.SemaphoreType.DMA((RECVS,)),
        pltpu.SemaphoreType.REGULAR((PAIR, PAIR)),
    ]
    up = jax.ShapeDtypeStruct((PAIR, LANE, LANE), F32)
    down = jax.ShapeDtypeStruct((PAIR, SUB, WIDE), F32)
    mau, mad, mou, mod, vau, vad = states
    grad, norm, low = pl.pallas_call(
        kernel,
        out_shape=(jax.ShapeDtypeStruct((FOUR, LANE, LANE), F32), jax.ShapeDtypeStruct((EIGHT, LANE), F32), jax.ShapeDtypeStruct((FOUR, PAIR, FOUR, LANE, LANE), BF16)),
        in_specs=[anywhere] * 10 + [scalar] * PAIR,
        out_specs=(anywhere, anywhere, anywhere),
        scratch_shapes=scratch,
        compiler_params=pltpu.CompilerParams(collective_id=0, has_side_effects=True, vmem_limit_bytes=VMEM_LIMIT),
        name="fused_step",
    )(act_in, grad_out, w_up, w_down, mau, mou, vau, mad, mod, vad, *scalars)
    return pl.pallas_call(
        finish_kernel,
        out_shape=(jax.ShapeDtypeStruct((PAIR, WIDE, LANE), BF16), jax.ShapeDtypeStruct((PAIR, LANE, WIDE), BF16), up, down, up, down, up, down, jax.ShapeDtypeStruct((1, 1), F32)),
        in_specs=[near] * 9 + [scalar] * PAIR,
        out_specs=tuple([near] * 9),
        name="finish",
    )(grad, norm, low, *states, *scalars)


def solution(mesh):
    big = Mesh(mesh.devices.reshape(EIGHT, FOUR, FOUR, PAIR), ("z", "y", "x", "c"))
    model = ("z", "y")
    data = ("x", "c")
    spec_rows = P(data, None)
    spec_wup = P(None, None, model)
    spec_wdown = P(None, model, None)
    spec_sup = P(None, data, model)
    spec_sdown = P(None, model + data, None)
    spec_scalar = P(None)

    def local_step(act_in, grad_out, w_up, w_down, master_up, master_down, mom_up, mom_down, var_up, var_down, learn_rate, clip_norm):
        states = (master_up, master_down, mom_up, mom_down, var_up, var_down)
        outs = fused_step(act_in, grad_out, w_up, w_down, states, (learn_rate, clip_norm))
        return outs[:EIGHT] + (outs[EIGHT].reshape(1),)

    return jax.shard_map(local_step, mesh=big, in_specs=(spec_rows, spec_rows, spec_wup, spec_wdown, spec_sup, spec_sdown, spec_sup, spec_sdown, spec_sup, spec_sdown, spec_scalar, spec_scalar), out_specs=(spec_wup, spec_wdown, spec_sup, spec_sdown, spec_sup, spec_sdown, spec_sup, spec_sdown, spec_scalar), check_vma=False)
```

```python
import jax
import jax.numpy as jnp
from jax import lax
from jax.experimental import pallas as pl
from jax.experimental.pallas import tpu as pltpu
from jax.sharding import Mesh, PartitionSpec as P

STEP = 10
BETA_ONE = 0.9
BETA_TWO = 0.95
ADAM_EPS = 1e-8
NORM_EPS = 1e-6
F32 = jnp.float32
BF16 = jnp.bfloat16
MESH = pl.DeviceIdType.MESH
ROOT = 0.7978845608028654
CUBE = 0.044715
VMEM_LIMIT = 67043328
WIDE = 1024
LANE = 128
SPAN = 512
TILE = 256
HALF = 64
SUB = 16
EIGHT = 8
FOUR = 4
PAIR = 2
TRIO = 3
SEVEN = 7
HALFROW = 32
SIX = 6


def nn(left, right):
    return lax.dot_general(left, right, (((1,), (0,)), ((), ())), preferred_element_type=F32)


def nt(left, right):
    return lax.dot_general(left, right, (((1,), (1,)), ((), ())), preferred_element_type=F32)


def tn(left, right):
    return lax.dot_general(left, right, (((0,), (0,)), ((), ())), preferred_element_type=F32)


def gelu_val(z):
    t = jnp.tanh(ROOT * (z + CUBE * (z * z * z)))
    return z * (0.5 * (1.0 + t))


def gelu_both(z):
    sq = z * z
    t = jnp.tanh(ROOT * (z + CUBE * (sq * z)))
    half = 0.5 * (1.0 + t)
    slope = half + z * (0.5 * (1.0 - t * t)) * (ROOT * (1.0 + (3.0 * CUBE) * sq))
    return z * half, slope


def adam_update(master_arr, mom_arr, var_arr, grad_arr, clip_scale, lr_val):
    scaled = clip_scale * grad_arr
    new_mom = BETA_ONE * mom_arr + (1.0 - BETA_ONE) * scaled
    new_var = BETA_TWO * var_arr + (1.0 - BETA_TWO) * scaled * scaled
    mom_hat = new_mom / (1.0 - BETA_ONE ** STEP)
    var_hat = new_var / (1.0 - BETA_TWO ** STEP)
    new_master = master_arr - lr_val * mom_hat / (jnp.sqrt(var_hat) + ADAM_EPS)
    return new_master, new_mom, new_var


def kernel(
    act_ref, dy_ref, wup_ref, wdn_ref, up_ref_a, up_ref_b, up_ref_c, down_ref_a, down_ref_b, down_ref_c, lr_ref, clip_ref,
    grad_out_ref, norm_out_ref, weight_out_ref,
    X, DY, W, Z1, A1, Z3, A3, H, E2, Q3, PART, Y1, Y2, G, DD, X1, X2, ZS, ZR, NW, NSRC, NRCV, NRCW, SUP, SDN, GOUT, NOUT,
    local_sem, send_sem, recv_sem, credit,
):
    z = lax.axis_index("z")
    y = lax.axis_index("y")
    x = lax.axis_index("x")
    c = lax.axis_index("c")
    other = 1 - c
    used = {"send": 0, "recv": 0}

    def recv_id():
        used["recv"] += 1
        return used["recv"] - 1

    def send(src, dst, rid, where):
        sid = used["send"]
        used["send"] += 1
        copy = pltpu.make_async_remote_copy(src_ref=src, dst_ref=dst, send_sem=send_sem.at[sid], recv_sem=recv_sem.at[rid], device_id=where, device_id_type=MESH)
        copy.start()
        return copy

    def got(dst, rid):
        pltpu.make_async_remote_copy(src_ref=dst, dst_ref=dst, send_sem=send_sem.at[0], recv_sem=recv_sem.at[rid], device_id={"c": other}, device_id_type=MESH).wait_recv()

    places = [
        (wup_ref.at[0], Q3.at[0]),
        (act_ref.at[pl.ds(z * WIDE, WIDE), :], X),
        (wdn_ref.at[0], W.at[1, z]),
        (wup_ref.at[1], Q3.at[1]),
        (wdn_ref.at[1], W.at[TRIO, z]),
        (dy_ref.at[pl.ds(z * WIDE, WIDE), :], DY),
    ]
    for k, ref in enumerate((up_ref_a, up_ref_b, up_ref_c)):
        places.append((ref, SUP.at[k]))
    for k, ref in enumerate((down_ref_a, down_ref_b, down_ref_c)):
        places.append((ref, SDN.at[k]))
    loads = [pltpu.make_async_copy(src, dst, local_sem.at[i]) for i, (src, dst) in enumerate(places)]
    for copy in loads:
        copy.start()

    barrier = pltpu.get_barrier_semaphore()
    for d in range(1, EIGHT):
        pl.semaphore_signal(barrier, inc=1, device_id={"z": (z + d) % EIGHT}, device_id_type=MESH)
    flat_me = y * EIGHT + x * PAIR + c

    def flat_device(k):
        return {"y": k // EIGHT, "x": (k // PAIR) % FOUR, "c": k % PAIR}

    def flat_body(d, _):
        pl.semaphore_signal(barrier, inc=1, device_id=flat_device((flat_me + d) % HALFROW), device_id_type=MESH)
        return 0

    lax.fori_loop(1, HALFROW, flat_body, 0)

    zr, zl = (z + 1) % EIGHT, (z + SEVEN) % EIGHT

    class WRing:
        def __init__(self, m):
            self.m = m
            self.rids = [recv_id() for _ in range(FOUR)]
            self.lids = [recv_id() for _ in range(FOUR)]
            self.dids = [recv_id() for _ in range(SEVEN)]
            self.sent = []

        def piece(self, idx, lo=0, n=HALF):
            return W.at[self.m, idx, pl.ds(c * HALF + lo, n), :]

        def far(self, idx):
            return W.at[self.m, idx, pl.ds(other * HALF, HALF), :]

        def push(self, idx, lo, n, rid, where):
            p = self.piece(idx, lo, n)
            self.sent.append(send(p, p, rid, where))

        def start(self):
            self.push(z, 0, HALF, self.rids[0], {"z": zr})
            self.push(z, 0, HALF, self.lids[0], {"z": zl})

        def step(self, s):
            if s < TRIO:
                a, b = (z + SEVEN - s) % EIGHT, (z + 1 + s) % EIGHT
                got(self.piece(a), self.rids[s])
                if s < PAIR:
                    self.push(a, 0, HALF, self.rids[s + 1], {"z": zr})
                else:
                    self.push(a, 0, HALFROW, self.rids[TRIO], {"z": zr})
                self.push(a, 0, HALF, self.dids[PAIR * s], {"c": other})
                got(self.piece(b), self.lids[s])
                if s < PAIR:
                    self.push(b, 0, HALF, self.lids[s + 1], {"z": zl})
                else:
                    self.push(b, HALFROW, HALFROW, self.lids[TRIO], {"z": zl})
                self.push(b, 0, HALF, self.dids[PAIR * s + 1], {"c": other})
            else:
                a = (z + FOUR) % EIGHT
                got(self.piece(a, 0, HALFROW), self.rids[TRIO])
                got(self.piece(a, HALFROW, HALFROW), self.lids[TRIO])
                self.push(a, 0, HALF, self.dids[SIX], {"c": other})

        def near(self, s):
            if s < TRIO:
                a, b = (z + SEVEN - s) % EIGHT, (z + 1 + s) % EIGHT
                got(self.far(a), self.dids[PAIR * s])
                got(self.far(b), self.dids[PAIR * s + 1])
                return [a, b]
            a = (z + FOUR) % EIGHT
            got(self.far(a), self.dids[SIX])
            return [a]

    class FirstRing:
        def __init__(self):
            self.rids = [[recv_id() for _ in range(PAIR)] for _ in range(FOUR)]
            self.lids = [[recv_id() for _ in range(PAIR)] for _ in range(FOUR)]
            self.dids = [recv_id() for _ in range(SEVEN)]
            self.sent = []

        def piece(self, idx, u):
            return W.at[0, idx, pl.ds(c * HALF + u * HALFROW, HALFROW), :]

        def push(self, idx, u, rid, where):
            p = self.piece(idx, u)
            self.sent.append(send(p, p, rid, where))

        def cross(self, idx, rid):
            p = W.at[0, idx, pl.ds(c * HALF, HALF), :]
            self.sent.append(send(p, p, rid, {"c": other}))

        def start(self, u):
            self.push(z, u, self.rids[0][u], {"z": zr})
            self.push(z, u, self.lids[0][u], {"z": zl})

        def step(self, s):
            if s < TRIO:
                a, b = (z + SEVEN - s) % EIGHT, (z + 1 + s) % EIGHT
                for u in range(PAIR):
                    got(self.piece(a, u), self.rids[s][u])
                    if s < PAIR or u == 0:
                        self.push(a, u, self.rids[s + 1][u], {"z": zr})
                    got(self.piece(b, u), self.lids[s][u])
                    if s < PAIR or u == 1:
                        self.push(b, u, self.lids[s + 1][u], {"z": zl})
                self.cross(a, self.dids[PAIR * s])
                self.cross(b, self.dids[PAIR * s + 1])
            else:
                a = (z + FOUR) % EIGHT
                got(self.piece(a, 0), self.rids[s][0])
                got(self.piece(a, 1), self.lids[s][1])
                self.cross(a, self.dids[PAIR * s])

        def near(self, s):
            found = [(z + SEVEN - s) % EIGHT, (z + 1 + s) % EIGHT] if s < TRIO else [(z + FOUR) % EIGHT]
            for i, j in enumerate(found):
                got(W.at[0, j, pl.ds(other * HALF, HALF), :], self.dids[PAIR * s + i])
            return found

    class Rs4:
        def __init__(self, axis, me, src, one, two):
            self.axis, self.src, self.one, self.two = axis, src, one, two
            self.me, self.r, self.l, self.o = me, (me + 1) % FOUR, (me + TRIO) % FOUR, (me + PAIR) % FOUR
            self.ids = [recv_id() for _ in range(SIX)]
            self.sent = []

        def start(self):
            right, left = {self.axis: self.r}, {self.axis: self.l}
            self.sent.append(send(self.src(self.o, 0), self.one(0), self.ids[0], right))
            self.sent.append(send(self.src(self.o, 1), self.one(1), self.ids[1], left))
            self.sent.append(send(self.src(self.r, 1), self.two(0, 1), self.ids[TRIO], right))
            self.sent.append(send(self.src(self.l, 0), self.two(1, 0), self.ids[FOUR], left))

        def mid(self):
            got(self.one(0), self.ids[0])
            mine = self.src(self.r, 0)
            mine[...] = mine[...] + self.one(0)[...]
            self.sent.append(send(mine, self.two(0, 0), self.ids[PAIR], {self.axis: self.r}))
            got(self.one(1), self.ids[1])
            mine = self.src(self.l, 1)
            mine[...] = mine[...] + self.one(1)[...]
            self.sent.append(send(mine, self.two(1, 1), self.ids[5], {self.axis: self.l}))

        def fin(self, h):
            got(self.two(0, h), self.ids[PAIR + h])
            got(self.two(1, h), self.ids[FOUR + h])
            return self.src(self.me, h)[...] + self.two(0, h)[...] + self.two(1, h)[...]

    class Ag4:
        def __init__(self, axis, me, buf):
            self.axis, self.buf = axis, buf
            self.me, self.r, self.l, self.o = me, (me + 1) % FOUR, (me + TRIO) % FOUR, (me + PAIR) % FOUR
            self.ids = [recv_id() for _ in range(SIX)]
            self.sent = []

        def push(self, j, h, rid, to):
            p = self.buf(j, h)
            self.sent.append(send(p, p, rid, {self.axis: to}))

        def start(self):
            self.push(self.me, 0, self.ids[0], self.r)
            self.push(self.me, 1, self.ids[TRIO], self.l)
            self.push(self.me, 1, self.ids[1], self.r)
            self.push(self.me, 0, self.ids[PAIR], self.l)

        def fwd(self):
            got(self.buf(self.l, 0), self.ids[0])
            self.push(self.l, 0, self.ids[FOUR], self.r)
            got(self.buf(self.r, 1), self.ids[TRIO])
            self.push(self.r, 1, self.ids[5], self.l)

        def fin(self):
            got(self.buf(self.l, 1), self.ids[1])
            got(self.buf(self.r, 0), self.ids[PAIR])
            got(self.buf(self.o, 0), self.ids[FOUR])
            got(self.buf(self.o, 1), self.ids[5])

    class SharedRing:
        def __init__(self):
            self.rids = [recv_id() for _ in range(FOUR)]
            self.lids = [recv_id() for _ in range(TRIO)]
            self.dids = [recv_id() for _ in range(SEVEN)]
            self.sent = []
            self.ags = []
            for s in range(FOUR):
                if s < TRIO:
                    pair = ((z + SEVEN - s) % EIGHT, (z + 1 + s) % EIGHT)
                    self.ags.append(Ag4("x", x, lambda j, h, pair=pair: self.piece(pair[h], j)))
                else:
                    self.ags.append(Ag4("x", x, lambda j, h: W.at[1, (z + FOUR) % EIGHT, pl.ds(c * HALF + j * SUB + h * EIGHT, EIGHT), :]))

        def piece(self, idx, j):
            return W.at[1, idx, pl.ds(c * HALF + j * SUB, SUB), :]

        def push(self, idx, rid, where):
            p = self.piece(idx, x)
            self.sent.append(send(p, p, rid, where))

        def start(self):
            self.push(z, self.rids[0], {"z": zr})
            self.push(z, self.lids[0], {"z": zl})

        def step(self, s):
            a, b = (z + SEVEN - s) % EIGHT, (z + 1 + s) % EIGHT
            got(self.piece(a, x), self.rids[s])
            if s < TRIO:
                self.push(a, self.rids[s + 1], {"z": zr})
                got(self.piece(b, x), self.lids[s])
                if s < PAIR:
                    self.push(b, self.lids[s + 1], {"z": zl})
            self.ags[s].start()

        def fwd(self, s):
            self.ags[s].fwd()

        def chunks(self, s):
            return [(z + SEVEN - s) % EIGHT, (z + 1 + s) % EIGHT] if s < TRIO else [(z + FOUR) % EIGHT]

        def fin(self, s):
            self.ags[s].fin()
            for i, j in enumerate(self.chunks(s)):
                p = W.at[1, j, pl.ds(c * HALF, HALF), :]
                self.sent.append(send(p, p, self.dids[PAIR * s + i], {"c": other}))

        def near(self, s):
            for i, j in enumerate(self.chunks(s)):
                got(W.at[1, j, pl.ds(other * HALF, HALF), :], self.dids[PAIR * s + i])

    def done(*things):
        for thing in things:
            for copy in thing.sent:
                copy.wait_send()
            thing.sent = []

    def rows_of(ref, p):
        return ref[p].reshape(SPAN, WIDE)

    def first_slice(j):
        def body(i, _):
            rows = pl.ds(pl.multiple_of(i * TILE, TILE), TILE)
            low = nt(X[rows, :], W[0, j]).astype(BF16)
            Z1[j, rows, :] = low
            A1[j, rows, :] = gelu_val(low.astype(F32)).astype(BF16)
            return 0

        lax.fori_loop(0, FOUR, body, 0)

    def partial(p, lhs, m, slices, add):
        def body(n, _):
            cols = pl.ds(pl.multiple_of(n * TILE, TILE), TILE)
            right = jnp.concatenate([W[m, i, :, cols] for i in slices], axis=0)
            left = jnp.concatenate([lhs[i, p * SPAN:(p + 1) * SPAN, :] for i in slices], axis=1)
            val = nn(left, right).reshape(FOUR, LANE, TILE)
            PART[p, :, :, cols] = PART[p, :, :, cols] + val if add else val
            return 0

        lax.fori_loop(0, FOUR, body, 0)

    def err_three(p):
        def body(n, _):
            val = nt(DY[p * SPAN:(p + 1) * SPAN, :], W[TRIO, pl.ds(PAIR * n, PAIR)].reshape(TILE, WIDE)).astype(BF16)
            Q3[PAIR * n, p * SPAN:(p + 1) * SPAN, :] = val[:, :LANE]
            Q3[PAIR * n + 1, p * SPAN:(p + 1) * SPAN, :] = val[:, LANE:]
            return 0

        lax.fori_loop(0, FOUR, body, 0)

    def block_two(p):
        def body(n, _):
            low = nt(rows_of(H, p), W[PAIR, pl.ds(PAIR * n, PAIR)].reshape(TILE, WIDE)).astype(BF16)
            for k in range(PAIR):
                part = low[:, k * LANE:(k + 1) * LANE].astype(F32)
                val, slope = gelu_both(part)
                A3[PAIR * n + k, p * SPAN:(p + 1) * SPAN, :] = val.astype(BF16)
                err = Q3[PAIR * n + k, p * SPAN:(p + 1) * SPAN, :].astype(F32)
                Q3[PAIR * n + k, p * SPAN:(p + 1) * SPAN, :] = (err * slope).astype(BF16)
            return 0

        lax.fori_loop(0, FOUR, body, 0)

    def back_one(p):
        def body(n, _):
            low = nt(rows_of(E2, p), W[1, pl.ds(PAIR * n, PAIR)].reshape(TILE, WIDE)).astype(BF16)
            for k in range(PAIR):
                zed = Z1[PAIR * n + k, p * SPAN:(p + 1) * SPAN, :].astype(F32)
                _, slope = gelu_both(zed)
                err = low[:, k * LANE:(k + 1) * LANE].astype(F32)
                Z3[PAIR * n + k, p * SPAN:(p + 1) * SPAN, :] = (err * slope).astype(BF16)
            return 0

        lax.fori_loop(0, FOUR, body, 0)

    def weight_grad(slot, hid, lo, size, other_side, down, first, last, add):
        def body(step, _):
            n = step // PAIR
            half = step % PAIR
            cols = pl.ds(pl.multiple_of(n * TILE, TILE), TILE)
            right = other_side(cols)
            for q in range(PAIR):
                base = half * FOUR + q * PAIR
                left = jnp.concatenate([hid[base, lo:lo + size, :], hid[base + 1, lo:lo + size, :]], axis=1)
                val = tn(left, right)
                for k in range(PAIR):
                    blk = val[k * LANE:(k + 1) * LANE, :]
                    for e in range(PAIR):
                        sub = blk[:, e * LANE:(e + 1) * LANE]
                        if down:
                            lane = pl.ds(pl.multiple_of((PAIR * n + e) * SUB, SUB), SUB)
                            for b in range(EIGHT):
                                old = G[slot, base + k, b // PAIR, b % PAIR, lane, :] if add else 0.0
                                G[slot, base + k, b // PAIR, b % PAIR, lane, :] = old + sub[b * SUB:(b + 1) * SUB, :]
                        else:
                            old = G[slot, base + k, n, e] if add else 0.0
                            G[slot, base + k, n, e] = old + sub
            return 0

        lax.fori_loop(PAIR * first, PAIR * last, body, 0)

    class GradPart:
        def __init__(self, k, i, lo, size):
            self.k, self.i, self.slot, self.size = k, i, k % PAIR, size
            self.did = recv_id()
            self.zid = recv_id()
            slot = self.slot
            rows = pl.ds(lo, size)
            self.rows = rows
            self.rs = Rs4("x", x, lambda j, h: G.at[slot, pl.ds(FOUR * h, FOUR), j, c, rows], lambda d: X1.at[k, d, :, rows], lambda d, h: X2.at[k, d, h, :, rows])
            self.sent = []
            self.zsent = []

        def d2d(self):
            if self.k >= PAIR and self.i == 0:
                pl.semaphore_wait(credit.at[self.slot], PAIR)
            self.sent.append(send(G.at[self.slot, :, :, other, self.rows], DD.at[self.slot, :, :, self.rows], self.did, {"c": other}))

        def xs(self):
            slot, rows = self.slot, self.rows
            got(DD.at[slot, :, :, rows], self.did)

            def body(i, _):
                mine = G.at[slot, i, :, c, rows]
                mine[...] = mine[...] + DD[slot, i, :, rows]
                return 0

            lax.fori_loop(0, EIGHT, body, 0)
            if self.k < PAIR:
                pl.semaphore_signal(credit.at[slot], inc=1, device_id={"c": other}, device_id_type=MESH)
            self.rs.start()

        def xm(self):
            self.rs.mid()

        def xf(self):
            for h in range(PAIR):
                ZS[self.slot, FOUR * h:FOUR * h + FOUR, self.rows] = self.rs.fin(h)
            for d in (FOUR, TRIO, 5, PAIR, SIX, 1, SEVEN):
                to = (z + d) % EIGHT
                self.zsent.append(send(ZS.at[self.slot, to, self.rows], ZR.at[self.k, d - 1, self.rows], self.zid, {"z": to}))

        def zf(self):
            got(ZR.at[self.k, :, self.rows], self.zid)
            total = ZS[self.slot, z, self.rows]
            for d in range(SEVEN):
                total = total + ZR[self.k, d, self.rows]
            total = total * 0.125
            GOUT[self.k, self.rows, :] = total
            sq = total * total
            return jnp.sum(sq.reshape(self.size // EIGHT, EIGHT, LANE), axis=0)

        def free_g(self):
            done(self, self.rs)

        def free_z(self):
            for copy in self.zsent:
                copy.wait_send()
            self.zsent = []

    w1, w2, w3, w4 = FirstRing(), SharedRing(), WRing(PAIR), WRing(TRIO)
    every = tuple(range(EIGHT))
    rs_h = [Rs4("y", y, lambda j, h, p=p: PART.at[p, j, pl.ds(HALF * h, HALF), :], lambda d, p=p: Y1.at[0, p, d], lambda d, h, p=p: Y2.at[0, p, d, h]) for p in range(PAIR)]
    rs_e = [Rs4("y", y, lambda j, h, p=p: PART.at[p, j, pl.ds(HALF * h, HALF), :], lambda d, p=p: Y1.at[1, p, d], lambda d, h, p=p: Y2.at[1, p, d, h]) for p in range(PAIR)]
    ag_h = [Ag4("y", y, lambda j, h, p=p: H.at[p, j, pl.ds(HALF * h, HALF), :]) for p in range(PAIR)]
    ag_e = [Ag4("y", y, lambda j, h, p=p: E2.at[p, j, pl.ds(HALF * h, HALF), :]) for p in range(PAIR)]
    cuts = (
        ((0, HALF), (HALF, HALF)),
        ((0, HALF), (HALF, HALF)),
        ((0, HALFROW), (HALFROW, HALFROW), (HALF, HALF)),
        ((0, HALF), (HALF, HALFROW), (HALF + HALFROW, HALFROW)),
    )
    gs = [[GradPart(k, i, lo, size) for i, (lo, size) in enumerate(cuts[k])] for k in range(FOUR)]

    loads[0].wait()
    W[0, z] = Q3[0].T
    loads[1].wait()
    first_slice(z)
    loads[PAIR].wait()
    pl.semaphore_wait(barrier, 38)
    w2.start()
    w1.start(0)
    w1.start(1)
    loads[TRIO].wait()
    W[PAIR, z] = Q3[1].T
    loads[FOUR].wait()
    for s in range(FOUR):
        w2.step(s)
        w1.step(s)
        if s == PAIR:
            w3.start()
            w4.start()
        if s >= 1:
            w2.fwd(s - 1)
        if s >= PAIR:
            w2.fin(s - PAIR)
        for j in w1.near(s):
            first_slice(j)
    w2.fwd(TRIO)
    w2.fin(PAIR)
    for s in range(TRIO):
        w2.near(s)
    far = (z + FOUR) % EIGHT
    partial(0, A1, 1, [(z + d) % EIGHT for d in (0, 1, PAIR, TRIO, 5, SIX, SEVEN)], False)
    w2.fin(TRIO)
    w2.near(TRIO)
    partial(0, A1, 1, [far], True)
    rs_h[0].start()
    w3.step(0)
    w4.step(0)
    partial(1, A1, 1, every, False)
    rs_h[1].start()
    w3.step(1)
    w4.step(1)
    rs_h[0].mid()
    w3.step(PAIR)
    w4.step(PAIR)
    loads[5].wait()
    rs_h[1].mid()
    w3.step(TRIO)
    w4.step(TRIO)
    for s in range(FOUR):
        w4.near(s)
    err_three(0)
    for h in range(PAIR):
        H[0, y, HALF * h:HALF * h + HALF, :] = rs_h[0].fin(h).astype(BF16)
    ag_h[0].start()
    err_three(1)
    for s in range(FOUR):
        w3.near(s)
    for h in range(PAIR):
        H[1, y, HALF * h:HALF * h + HALF, :] = rs_h[1].fin(h).astype(BF16)
    ag_h[0].fwd()
    ag_h[1].start()
    ag_h[0].fin()
    block_two(0)
    ag_h[1].fwd()
    done(rs_h[0])
    partial(0, Q3, PAIR, every, False)
    rs_e[0].start()
    ag_h[1].fin()
    block_two(1)
    done(rs_h[1])
    partial(1, Q3, PAIR, every, False)
    rs_e[1].start()
    rs_e[0].mid()
    weight_grad(0, A3, 0, WIDE, lambda cols: DY[:, cols], True, 0, PAIR, False)
    gs[0][0].d2d()
    weight_grad(0, A3, 0, WIDE, lambda cols: DY[:, cols], True, PAIR, FOUR, False)
    gs[0][1].d2d()
    gs[0][0].xs()
    weight_grad(1, Q3, 0, WIDE, lambda cols: H[:, :, :, cols].reshape(WIDE, TILE), False, 0, FOUR, False)
    gs[0][1].xs()
    gs[1][0].d2d()
    gs[1][1].d2d()
    rs_e[1].mid()
    gs[0][0].xm()
    gs[0][1].xm()
    gs[1][0].xs()
    gs[1][1].xs()
    for h in range(PAIR):
        E2[0, y, HALF * h:HALF * h + HALF, :] = rs_e[0].fin(h).astype(BF16)
    ag_e[0].start()
    gs[0][0].xf()
    gs[0][1].xf()
    for h in range(PAIR):
        E2[1, y, HALF * h:HALF * h + HALF, :] = rs_e[1].fin(h).astype(BF16)
    ag_e[0].fwd()
    ag_e[1].start()
    gs[1][0].xm()
    gs[1][1].xm()
    gs[0][0].free_g()
    gs[0][1].free_g()
    ag_e[0].fin()
    back_one(0)
    ag_e[1].fwd()
    weight_grad(0, A1, 0, SPAN, lambda cols: E2[0, :, :, cols].reshape(SPAN, TILE), True, 0, FOUR, False)
    gs[1][0].xf()
    gs[1][1].xf()
    gs[1][0].free_g()
    gs[1][1].free_g()
    weight_grad(1, Z3, 0, SPAN, lambda cols: X[:SPAN, cols], False, 0, FOUR, False)
    ag_e[1].fin()

    def second(cols):
        return E2[1, :, :, cols].reshape(SPAN, TILE)

    weight_grad(0, A1, SPAN, SPAN, second, True, 0, 1, True)
    gs[PAIR][0].d2d()
    weight_grad(0, A1, SPAN, SPAN, second, True, 1, PAIR, True)
    gs[PAIR][1].d2d()
    weight_grad(0, A1, SPAN, SPAN, second, True, PAIR, FOUR, True)
    gs[PAIR][PAIR].d2d()
    gs[PAIR][0].xs()
    gs[PAIR][1].xs()
    back_one(1)
    gs[PAIR][PAIR].xs()
    weight_grad(1, Z3, SPAN, SPAN, lambda cols: X[SPAN:, cols], False, 0, FOUR, True)
    for part in gs[TRIO]:
        part.d2d()
    gs[PAIR][0].xm()
    gs[PAIR][1].xm()
    gs[TRIO][0].xs()
    gs[PAIR][PAIR].xm()
    gs[TRIO][1].xs()
    gs[TRIO][PAIR].xs()
    sq = gs[0][0].zf() + gs[0][1].zf()
    gs[0][0].free_z()
    gs[0][1].free_z()
    gs[PAIR][0].xf()
    gs[PAIR][1].xf()
    gs[TRIO][0].xm()
    gs[PAIR][PAIR].xf()
    gs[TRIO][1].xm()
    gs[TRIO][PAIR].xm()
    sq = sq + gs[1][0].zf() + gs[1][1].zf()
    gs[1][0].free_z()
    gs[1][1].free_z()
    gs[TRIO][0].xf()
    sq = sq + gs[PAIR][0].zf() + gs[PAIR][1].zf()
    gs[TRIO][1].xf()
    gs[TRIO][PAIR].xf()
    sq = sq + gs[PAIR][PAIR].zf() + gs[TRIO][0].zf()
    sq = sq + gs[TRIO][1].zf()
    sq = sq + gs[TRIO][PAIR].zf()

    grad_copy = pltpu.make_async_copy(GOUT, grad_out_ref, local_sem.at[0])
    grad_copy.start()
    nid, mid = recv_id(), recv_id()
    norm_sent = []
    NSRC[0] = sq
    for d in (FOUR, TRIO, 5, PAIR, SIX, 1, SEVEN):
        norm_sent.append(send(NSRC.at[0], NRCV.at[z], nid, {"z": (z + d) % EIGHT}))
    got(NRCV.at[pl.ds(0, SEVEN)], nid)
    NRCV[z] = sq
    part = NRCV[0]
    for k in range(1, EIGHT):
        part = part + NRCV[k]
    row = jnp.sum(part, axis=0, keepdims=True)
    row = jnp.broadcast_to(row, (EIGHT, LANE))
    NSRC[1] = row
    for d in range(1, HALFROW):
        norm_sent.append(send(NSRC.at[1], NRCW.at[flat_me], mid, flat_device((flat_me + d) % HALFROW)))
    got(NRCW.at[pl.ds(0, 31)], mid)
    NRCW[flat_me] = row
    total = jnp.sum(jnp.sum(NRCW[...], axis=0)[:1, :], axis=1, keepdims=True)
    norm_val = jnp.sqrt(total)
    NOUT[...] = jnp.broadcast_to(norm_val, (EIGHT, LANE))
    norm_copy = pltpu.make_async_copy(NOUT, norm_out_ref, local_sem.at[1])
    norm_copy.start()
    clip_scale = jnp.minimum(1.0, clip_ref[0] / (norm_val + NORM_EPS))
    lr_val = lr_ref[0]
    for copy in loads[SIX:]:
        copy.wait()
    for k in range(PAIR):
        new_master, _, _ = adam_update(SUP[0, k], SUP[1, k], SUP[PAIR, k], GOUT[TRIO - PAIR * k].T, clip_scale, lr_val)
        NW[x, c, k] = new_master.astype(BF16)
        flat = flatten(GOUT[PAIR - PAIR * k])
        new_master, _, _ = adam_update(SDN[0, k], SDN[1, k], SDN[PAIR, k], flat, clip_scale, lr_val)
        low = new_master.astype(BF16)
        for e in range(EIGHT):
            NW[x, c, PAIR + k, e * SUB:(e + 1) * SUB, :] = low[:, e * LANE:(e + 1) * LANE]
    ag_w = Ag4("x", x, lambda j, h: NW.at[j, c, pl.ds(PAIR * h, PAIR)])
    ag_w.start()
    pair = [recv_id() for _ in range(FOUR)]
    last = []

    def across(i, j):
        last.append(send(NW.at[j, c], NW.at[j, c], pair[i], {"c": other}))

    across(0, x)
    ag_w.fwd()
    ag_w.fin()
    for i, j in ((1, ag_w.l), (PAIR, ag_w.r), (TRIO, ag_w.o)):
        across(i, j)
    for i, j in ((0, x), (1, ag_w.l), (PAIR, ag_w.r), (TRIO, ag_w.o)):
        got(NW.at[j, other], pair[i])
    weight_copy = pltpu.make_async_copy(NW, weight_out_ref, local_sem.at[PAIR])
    weight_copy.start()

    for copy in last + norm_sent:
        copy.wait_send()
    done(w1, w2, w3, w4, ag_w, *w2.ags, *rs_e, *ag_h, *ag_e)
    for parts in gs[PAIR:]:
        for part in parts:
            part.free_g()
            part.free_z()
    for copy in (grad_copy, norm_copy, weight_copy):
        copy.wait()


def flatten(grad):
    return jnp.concatenate([grad[e * SUB:(e + 1) * SUB, :] for e in range(EIGHT)], axis=1)


def finish_kernel(grad, norm, low, mau, mad, mou, mod, vau, vad, lr_ref, clip_ref, nwu, nwd, omau, omad, omou, omod, ovau, ovad, onorm):
    norm_val = norm[:1, :1]
    onorm[...] = norm_val
    clip_scale = jnp.minimum(1.0, clip_ref[0] / (norm_val + NORM_EPS))
    lr_val = lr_ref[0]
    for k in range(PAIR):
        omau[k], omou[k], ovau[k] = adam_update(mau[k], mou[k], vau[k], grad[TRIO - PAIR * k].T, clip_scale, lr_val)
        omad[k], omod[k], ovad[k] = adam_update(mad[k], mod[k], vad[k], flatten(grad[PAIR - PAIR * k]), clip_scale, lr_val)
        for b in range(EIGHT):
            nwu[k, b * LANE:(b + 1) * LANE, :] = low[b // PAIR, b % PAIR, k]
            nwd[k, b * SUB:(b + 1) * SUB, :] = flatten(low[b // PAIR, b % PAIR, PAIR + k])


SENDS = 420
RECVS = 330


def fused_step(act_in, grad_out, w_up, w_down, states, scalars):
    anywhere = pl.BlockSpec(memory_space=pl.ANY)
    near = pl.BlockSpec(memory_space=pltpu.VMEM)
    scalar = pl.BlockSpec(memory_space=pltpu.SMEM)
    act = pltpu.VMEM((EIGHT, WIDE, LANE), BF16)
    rows = pltpu.VMEM((PAIR, FOUR, LANE, WIDE), BF16)
    scratch = [
        pltpu.VMEM((WIDE, WIDE), BF16),
        pltpu.VMEM((WIDE, WIDE), BF16),
        pltpu.VMEM((FOUR, EIGHT, LANE, WIDE), BF16),
        act, act, act, act,
        rows, rows,
        act,
        pltpu.VMEM((PAIR, FOUR, LANE, WIDE), F32),
        pltpu.VMEM((PAIR, PAIR, PAIR, HALF, WIDE), F32),
        pltpu.VMEM((PAIR, PAIR, PAIR, PAIR, HALF, WIDE), F32),
        pltpu.VMEM((PAIR, EIGHT, FOUR, PAIR, LANE, LANE), F32),
        pltpu.VMEM((PAIR, EIGHT, FOUR, LANE, LANE), F32),
        pltpu.VMEM((FOUR, PAIR, FOUR, LANE, LANE), F32),
        pltpu.VMEM((FOUR, PAIR, PAIR, FOUR, LANE, LANE), F32),
        pltpu.VMEM((PAIR, EIGHT, LANE, LANE), F32),
        pltpu.VMEM((FOUR, SEVEN, LANE, LANE), F32),
        pltpu.VMEM((FOUR, PAIR, FOUR, LANE, LANE), BF16),
        pltpu.VMEM((PAIR, EIGHT, LANE), F32),
        pltpu.VMEM((EIGHT, EIGHT, LANE), F32),
        pltpu.VMEM((HALFROW, EIGHT, LANE), F32),
        pltpu.VMEM((TRIO, PAIR, LANE, LANE), F32),
        pltpu.VMEM((TRIO, PAIR, SUB, WIDE), F32),
        pltpu.VMEM((FOUR, LANE, LANE), F32),
        pltpu.VMEM((EIGHT, LANE), F32),
        pltpu.SemaphoreType.DMA((12,)),
        pltpu.SemaphoreType.DMA((SENDS,)),
        pltpu.SemaphoreType.DMA((RECVS,)),
        pltpu.SemaphoreType.REGULAR((PAIR,)),
    ]
    up = jax.ShapeDtypeStruct((PAIR, LANE, LANE), F32)
    down = jax.ShapeDtypeStruct((PAIR, SUB, WIDE), F32)
    mau, mad, mou, mod, vau, vad = states
    grad, norm, low = pl.pallas_call(
        kernel,
        out_shape=(jax.ShapeDtypeStruct((FOUR, LANE, LANE), F32), jax.ShapeDtypeStruct((EIGHT, LANE), F32), jax.ShapeDtypeStruct((FOUR, PAIR, FOUR, LANE, LANE), BF16)),
        in_specs=[anywhere] * 10 + [scalar] * PAIR,
        out_specs=(anywhere, anywhere, anywhere),
        scratch_shapes=scratch,
        compiler_params=pltpu.CompilerParams(collective_id=0, has_side_effects=True, vmem_limit_bytes=VMEM_LIMIT),
        name="fused_step",
    )(act_in, grad_out, w_up, w_down, mau, mou, vau, mad, mod, vad, *scalars)
    return pl.pallas_call(
        finish_kernel,
        out_shape=(jax.ShapeDtypeStruct((PAIR, WIDE, LANE), BF16), jax.ShapeDtypeStruct((PAIR, LANE, WIDE), BF16), up, down, up, down, up, down, jax.ShapeDtypeStruct((1, 1), F32)),
        in_specs=[near] * 9 + [scalar] * PAIR,
        out_specs=tuple([near] * 9),
        name="finish",
    )(grad, norm, low, *states, *scalars)


def solution(mesh):
    big = Mesh(mesh.devices.reshape(EIGHT, FOUR, FOUR, PAIR), ("z", "y", "x", "c"))
    model = ("z", "y")
    data = ("x", "c")
    spec_rows = P(data, None)
    spec_wup = P(None, None, model)
    spec_wdown = P(None, model, None)
    spec_sup = P(None, data, model)
    spec_sdown = P(None, model + data, None)
    spec_scalar = P(None)

    def local_step(act_in, grad_out, w_up, w_down, master_up, master_down, mom_up, mom_down, var_up, var_down, learn_rate, clip_norm):
        states = (master_up, master_down, mom_up, mom_down, var_up, var_down)
        outs = fused_step(act_in, grad_out, w_up, w_down, states, (learn_rate, clip_norm))
        return outs[:EIGHT] + (outs[EIGHT].reshape(1),)

    return jax.shard_map(local_step, mesh=big, in_specs=(spec_rows, spec_rows, spec_wup, spec_wdown, spec_sup, spec_sdown, spec_sup, spec_sdown, spec_sup, spec_sdown, spec_scalar, spec_scalar), out_specs=(spec_wup, spec_wdown, spec_sup, spec_sdown, spec_sup, spec_sdown, spec_sup, spec_sdown, spec_scalar), check_vma=False)
```
